32 devices in a mesh: groups: 2 (over y), tm: 4 (over z), section: 4 (over x, core).
Axes of the slice: x: 2, y: 2, z: 4, core: 2. Of those that a mesh axis runs over, the one named last changes fastest.
Arguments:
- states: float32 [16, 1, 4096], P(('groups', 'tm')), parts along dimension 0, may hold values from -6 to 6
- timesteps: int32 [16], P(('groups', 'tm')), parts along dimension 0, may hold values from 0 to 999
- step_sizes: float32 [16], P(('groups', 'tm')), parts along dimension 0, may hold values from 0.05 to 0.2
- labels: int32 [2], P('groups'), parts along dimension 0, may hold values from 0 to 1000
- class_table: bfloat16 [1001, 1152], replicated, may hold values from -6 to 6
- embed_weight: bfloat16 [16, 1152], replicated, may hold values from -1.5 to 1.5
- ada_weight: bfloat16 [4, 1152, 2304], P('section', 'tm'), may hold values from -0.1875 to 0.1875
- up_weight: bfloat16 [4, 1152, 2304], P('section', 'tm'), may hold values from -0.1875 to 0.1875
- down_weight: bfloat16 [4, 2304, 1152], P('section', 'tm'), may hold values from -0.125 to 0.125
- final_weight: bfloat16 [1152, 16], replicated, may hold values from -0.1875 to 0.1875
Outputs:
- new_states: float32 [16, 1, 4096], P(('groups', 'tm'), None, 'section'), parts along dimension 0
- step_err: float32 [16], P(('groups', 'tm')), parts along dimension 0
The draws below stay inside these ranges and needn't reach their ends.
There are 2 independent parts, one for each index of `groups`. The reference program is written for one: setup_inputs(seed, part) draws one part's arguments, and reference() takes and returns one part's arrays. A program takes and returns all parts, laid end to end along the dimension named above; an argument that names none is the same for every part. Nothing has to cross between parts.
All inputs are finite; a program needn't handle non-finite values.
Results may differ from the reference program's by a relative error of at most 0.0065.
Values may be sent and summed in bfloat16 or wider, within the bound.
No kernel may reach another device: no remote copies, remote signals or barrier semaphores. Data moves between devices by JAX's collectives and lax.ppermute only.
A program may use at most 128 MiB of HBM per device.

```python
import math
import jax
import jax.numpy as jnp
from jax import lax

D = 1152
PATCHES = 256
PCH = 16
CLASSES = 1001
FF = 2304
BATCH = 1
WINDOW = 8
LAYERS = 4
P_SIZE = 4096


def touch_ends(result, own_key, smallest, largest):
    longest = result.shape.index(max(result.shape))
    spots = []
    for shift in (0, 1):
        where = [jax.random.randint(jax.random.fold_in(own_key, axis), (), 0, length) for axis, length in enumerate(result.shape)]
        where[longest] = (where[longest] + shift) % result.shape[longest]
        spots.append(tuple(where))
    return result.at[spots[0]].set(smallest).at[spots[1]].set(largest)


def block_levels(rng, shape, split, smallest, largest):
    level = 1.0
    for dim, shards_of in split:
        draws = jax.random.uniform(jax.random.fold_in(jax.random.fold_in(rng, 6), dim), (shards_of,), jnp.float32, smallest / len(split), largest / len(split))
        level = level * jnp.repeat(jnp.exp(draws), shape[dim] // shards_of).reshape((-1,) + (1,) * (len(shape) - 1 - dim))
    return level


def noise(key, extent, scale, reach, cuts=(), kind=jnp.bfloat16):
    entries = jax.random.normal(key, extent, jnp.float32) * scale
    if len(cuts) > 0:
        entries = block_levels(key, extent, cuts, -0.22, 0.18) * entries
    return jnp.clip(entries, min=-reach, max=reach).astype(kind)


def setup_inputs(seed: int = 0, part: int = 0) -> dict:
    keys = jax.random.split(jax.random.key(seed), 11)
    part_splits = jax.random.split(jax.random.fold_in(keys[10], part), 11)
    states = noise(part_splits[0], (WINDOW, BATCH, P_SIZE), 1.0, 6.0, ((0, 4),), jnp.float32)
    timesteps = touch_ends(jax.random.randint(part_splits[1], (WINDOW,), 0, 1000), jax.random.fold_in(part_splits[1], 1), 0, 999).astype(jnp.int32)
    step_sizes = jnp.clip(jnp.exp(math.log(0.2) - 1.3862944 * jax.random.uniform(part_splits[2], (WINDOW,), jnp.float32) ** block_levels(part_splits[2], (WINDOW,), ((0, 4),), -0.2, 0.2)), 0.05, 0.2)
    labels = jax.random.randint(part_splits[3], (BATCH,), 0, CLASSES).astype(jnp.int32)
    class_table = noise(keys[4], (CLASSES, D), 1.0, 6.0)
    embed_weight = noise(keys[5], (PCH, D), PCH ** -0.5, 1.5)
    ada_weight = noise(keys[6], (LAYERS, D, 2 * D), D ** -0.5, 0.1875, ((0, 4), (1, 4)))
    up_weight = noise(keys[7], (LAYERS, D, FF), D ** -0.5, 0.1875, ((0, 4), (1, 4)))
    down_weight = noise(keys[8], (LAYERS, FF, D), FF ** -0.5, 0.125, ((0, 4), (1, 4)))
    final_weight = noise(keys[9], (D, PCH), D ** -0.5, 0.1875)
    return dict(states=states, timesteps=timesteps, step_sizes=step_sizes, labels=labels, class_table=class_table, embed_weight=embed_weight, ada_weight=ada_weight, up_weight=up_weight, down_weight=down_weight, final_weight=final_weight)


def condition_rows(timesteps, labels, class_table):
    half_width = D // 2
    frequency = jnp.exp(-math.log(10000.0) * jnp.arange(half_width, dtype=jnp.float32) / half_width)
    phases = timesteps.astype(jnp.float32)[:, None] * frequency[None, :]
    timing = jnp.concatenate([jnp.cos(phases), jnp.sin(phases)], axis=1)
    classes = class_table[labels].astype(jnp.float32)
    return jax.nn.silu(timing[:, None, :] + classes[None, :, :]).astype(jnp.bfloat16)

def normalize(values):
    center = values - lax.optimization_barrier(jnp.mean(values, axis=-1, keepdims=True))
    spread = lax.optimization_barrier(jnp.mean(center * center, axis=-1, keepdims=True))
    return center * jax.lax.rsqrt(spread + 1e-06)

def apply_layer(hidden, scale_mod, gate_mod, up_proj, down_proj):
    normed = (normalize(hidden) * (1.0 + scale_mod[:, None, :])).astype(jnp.bfloat16)
    inner = jax.nn.gelu(jnp.dot(normed.reshape(-1, D), up_proj, preferred_element_type=jnp.float32), approximate=True).astype(jnp.bfloat16)
    branch = jnp.dot(inner, down_proj, preferred_element_type=jnp.float32).reshape(hidden.shape)
    return (hidden + gate_mod[:, None, :] * branch).astype(jnp.bfloat16)

def reference(states, timesteps, step_sizes, labels, class_table, embed_weight, ada_weight, up_weight, down_weight, final_weight):
    row_total = WINDOW * BATCH
    cond_rows = condition_rows(timesteps, labels, class_table).reshape(row_total, D)
    patches = states.reshape(row_total, PATCHES, PCH).astype(jnp.bfloat16)
    hidden = jnp.dot(patches.reshape(-1, PCH), embed_weight, preferred_element_type=jnp.float32).reshape(row_total, PATCHES, D)
    for layer in range(LAYERS):
        modulation = jnp.dot(cond_rows, ada_weight[layer], preferred_element_type=jnp.float32)
        hidden = apply_layer(hidden, modulation[:, :D], modulation[:, D:], up_weight[layer], down_weight[layer]).astype(jnp.float32)
    normed = normalize(hidden).astype(jnp.bfloat16)
    drift_rows = jnp.dot(normed.reshape(-1, D), final_weight, preferred_element_type=jnp.float32).reshape(WINDOW, BATCH, P_SIZE)
    term_rows = step_sizes[:, None, None] * drift_rows
    running = jnp.cumsum(term_rows, axis=0)
    earlier = jnp.concatenate([jnp.zeros((1, BATCH, P_SIZE), jnp.float32), running[:-1]], axis=0)
    new_states = states[0][None] + earlier
    step_err = lax.optimization_barrier(jnp.max(jnp.abs(new_states - states), axis=(1, 2)))
    return (new_states, step_err)
```

```python
import math

import jax
import jax.numpy as jnp
from jax import lax
from jax.sharding import PartitionSpec as P

D = 1152
PATCHES = 256
PCH = 16
P_SIZE = 4096


def condition_rows(timesteps, labels, class_table):
    half_width = D // 2
    frequency = jnp.exp(-math.log(10000.0) * jnp.arange(half_width, dtype=jnp.float32) / half_width)
    phases = timesteps.astype(jnp.float32)[:, None] * frequency[None, :]
    timing = jnp.concatenate([jnp.cos(phases), jnp.sin(phases)], axis=1)
    classes = class_table[labels].astype(jnp.float32)
    return jax.nn.silu(timing[:, None, :] + classes[None, :, :]).astype(jnp.bfloat16)


def normalize(values):
    center = values - jnp.mean(values, axis=-1, keepdims=True)
    spread = jnp.mean(center * center, axis=-1, keepdims=True)
    return center * lax.rsqrt(spread + 1e-06)


def apply_layer(hidden, scale_mod, gate_mod, up_proj, down_proj):
    normed = (normalize(hidden) * (1.0 + scale_mod)).astype(jnp.bfloat16)
    inner = jax.nn.gelu(
        jnp.dot(normed, up_proj, preferred_element_type=jnp.float32), approximate=True
    ).astype(jnp.bfloat16)
    branch = jnp.dot(inner, down_proj, preferred_element_type=jnp.float32)
    return (hidden + gate_mod * branch).astype(jnp.bfloat16)


def gathered_weights(weights):
    tm = lax.axis_size("tm")
    groups = lax.axis_size("groups")
    if groups != 2 or tm > 8:
        return [lax.all_gather(w, "tm", axis=0, tiled=True) for w in weights]
    place = lax.axis_index("tm")
    mine = lax.axis_index("groups")
    halves = [w.reshape(2, w.shape[0] // 2, w.shape[1]) for w in weights]
    own = [lax.dynamic_index_in_dim(h, mine, 0, False) for h in halves]
    other = [lax.dynamic_index_in_dim(h, 1 - mine, 0, False) for h in halves]
    full = [
        lax.dynamic_update_slice(
            jnp.zeros((tm,) + h.shape, h.dtype), h[None], (place, 0, 0, 0)
        )
        for h in halves
    ]

    def put(index, piece, fallback, slot, valid, half):
        piece = jnp.where(valid, piece, fallback)
        slot = jnp.where(valid, slot, place)
        full[index] = lax.dynamic_update_slice(full[index], piece[None, None], (slot, half, 0, 0))

    ahead, behind = list(own), list(own)
    for k in range(1, tm):
        right = [(i, i + 1) for i in range(k - 1, tm - 1)]
        left = [(i + 1, i) for i in range(tm - k)]
        right_ends = [j for _, j in right]
        left_ends = [j for _, j in left]
        swap_right = [(g * tm + j, (1 - g) * tm + j) for g in range(2) for j in right_ends]
        swap_left = [(g * tm + j, (1 - g) * tm + j) for g in range(2) for j in left_ends]
        for w in range(len(weights)):
            ahead[w] = lax.ppermute(ahead[w], "tm", right)
            behind[w] = lax.ppermute(behind[w], "tm", left)
            ahead_y = lax.ppermute(ahead[w], ("groups", "tm"), swap_right)
            behind_y = lax.ppermute(behind[w], ("groups", "tm"), swap_left)
            has_right = place >= k
            has_left = place + k < tm
            put(w, ahead[w], own[w], place - k, has_right, mine)
            put(w, behind[w], own[w], place + k, has_left, mine)
            put(w, ahead_y, other[w], place - k, has_right, 1 - mine)
            put(w, behind_y, other[w], place + k, has_left, 1 - mine)
    return [f.reshape(-1, f.shape[-1]) for f in full]


def modulation_rows(cond_rows, ada_weight):
    tm = lax.axis_size("tm")
    place = lax.axis_index("tm")
    rows = cond_rows.shape[0]
    width = ada_weight.shape[0]

    def piece(t):
        return lax.dynamic_slice(cond_rows, (0, t * width), (rows, width))

    came = [piece(place)]
    for j in range(1, tm):
        ring = [(i, (i + j) % tm) for i in range(tm)]
        came.append(lax.ppermute(piece((place + j) % tm), "tm", ring))
    partial = jnp.dot(
        jnp.concatenate(came, axis=0), ada_weight, preferred_element_type=jnp.float32
    ).reshape(tm, rows, -1)
    total = partial[0]
    for j in range(1, tm):
        total = total + lax.ppermute(partial[j], "tm", [((i + j) % tm, i) for i in range(tm)])
    return total


def shards(
    states,
    timesteps,
    step_sizes,
    labels,
    class_table,
    embed_weight,
    ada_weight,
    up_weight,
    down_weight,
    final_weight,
):
    steps_here, batch_here = states.shape[:2]
    row_total = steps_here * batch_here
    section_idx = lax.axis_index("section")
    sections = lax.axis_size("section")
    tm = lax.axis_size("tm")
    last = sections - 1
    cond_rows = condition_rows(timesteps, labels, class_table).reshape(row_total, D)
    modulation = modulation_rows(cond_rows, ada_weight[0])
    up_proj, down_proj = gathered_weights([up_weight[0], down_weight[0]])
    scale_mod = modulation[:, :D]
    gate_mod = modulation[:, D:]

    first_state = jnp.where(lax.axis_index("tm") == 0, states[0], jnp.zeros_like(states[0]))
    own_first = first_state
    for j in range(1, tm):
        first_state = first_state + lax.ppermute(own_first, "tm", [(0, j)])

    patches = states.reshape(row_total, PATCHES, PCH).astype(jnp.bfloat16)
    embedded = jnp.dot(
        patches.reshape(-1, PCH), embed_weight, preferred_element_type=jnp.float32
    ).reshape(row_total, PATCHES, D)

    received = jnp.zeros((PATCHES, D), jnp.bfloat16)
    finished = []
    for tick in range(sections + row_total - 1):
        block = jnp.clip(tick - section_idx, 0, row_total - 1)
        entering = jnp.where(
            section_idx == 0, embedded[min(tick, row_total - 1)], received.astype(jnp.float32)
        )
        scale_row = lax.dynamic_slice_in_dim(scale_mod, block, 1, 0)
        gate_row = lax.dynamic_slice_in_dim(gate_mod, block, 1, 0)
        leaving = apply_layer(entering, scale_row, gate_row, up_proj, down_proj)
        if tick >= last:
            finished.append(leaving)
        pairs = [(s, s + 1) for s in range(last) if 0 <= tick - s < row_total]
        if pairs:
            received = lax.ppermute(leaving, "section", pairs)
    final = jnp.concatenate(finished, axis=0)
    normed = normalize(final.astype(jnp.float32)).astype(jnp.bfloat16)
    drift = jnp.dot(normed, final_weight, preferred_element_type=jnp.float32)
    drift = drift.reshape(steps_here, batch_here, P_SIZE)

    term_rows = step_sizes[:, None, None] * drift
    earlier = [jnp.zeros_like(term_rows[0])]
    for k in range(steps_here):
        earlier.append(earlier[-1] + term_rows[k])
    offset = first_state
    for j in range(1, tm):
        pairs = [(i * sections + last, (i + j) * sections + last) for i in range(tm - j)]
        offset = offset + lax.ppermute(earlier[-1], ("tm", "section"), pairs)
    new_states = offset[None] + jnp.stack(earlier[:-1])
    step_err = jnp.max(jnp.abs(new_states - states), axis=(1, 2))

    cols = P_SIZE // sections
    err_cols = jnp.broadcast_to(step_err[:, None, None], (steps_here, batch_here, 128))

    def packed(s):
        return jnp.concatenate([new_states[:, :, s * cols : (s + 1) * cols], err_cols], axis=2)

    out = jnp.where(section_idx == last, packed(last), 0.0)
    for s in range(last):
        out = out + lax.ppermute(packed(s), "section", [(last, s)])
    return (out[:, :, :cols], out[:, 0, cols])


def solution(mesh):
    return jax.shard_map(
        shards,
        mesh=mesh,
        in_specs=(
            P(("groups", "tm"), None, None),
            P(("groups", "tm")),
            P(("groups", "tm")),
            P("groups"),
            P(),
            P(),
            P("section", "tm", None),
            P("section", "tm", None),
            P("section", "tm", None),
            P(),
        ),
        out_specs=(P(("groups", "tm"), None, "section"), P(("groups", "tm"))),
        check_vma=False,
    )
```

```python
import math

import jax
import jax.numpy as jnp
from jax import lax
from jax.experimental import pallas as pl
from jax.experimental.pallas import tpu as pltpu
from jax.sharding import PartitionSpec as P

D = 1152
PATCHES = 256
PCH = 16
P_SIZE = 4096


def condition_rows(timesteps, labels, class_table):
    half_width = D // 2
    frequency = jnp.exp(-math.log(10000.0) * jnp.arange(half_width, dtype=jnp.float32) / half_width)
    phases = timesteps.astype(jnp.float32)[:, None] * frequency[None, :]
    timing = jnp.concatenate([jnp.cos(phases), jnp.sin(phases)], axis=1)
    classes = class_table[labels].astype(jnp.float32)
    return jax.nn.silu(timing[:, None, :] + classes[None, :, :]).astype(jnp.bfloat16)


def normalize(values):
    center = values - jnp.mean(values, axis=-1, keepdims=True)
    spread = jnp.mean(center * center, axis=-1, keepdims=True)
    return center * lax.rsqrt(spread + 1e-06)


def chunk_width(total, most):
    return max(w for w in range(128, most + 1, 128) if total % w == 0)


def layer_tick(first, patches, received, embed_weight, scale, gate, up_proj, down_proj, final_weight, with_drift):
    tokens, width = received.shape
    hidden_units = up_proj.shape[1]
    chunk = chunk_width(hidden_units, 768)
    steps = hidden_units // chunk

    def kernel(first_ref, patch_ref, recv_ref, embed_ref, scale_ref, gate_ref, up_ref, down_ref, fin_ref, out_ref, *rest):
        hid_ref, norm_ref, acc_ref = rest[-3:]
        j = pl.program_id(0)

        @pl.when(j == 0)
        def _():
            embedded = jnp.dot(patch_ref[...], embed_ref[...], preferred_element_type=jnp.float32)
            hidden = jnp.where(first_ref[0] == 1, embedded, recv_ref[...].astype(jnp.float32))
            hid_ref[...] = hidden
            norm_ref[...] = (normalize(hidden) * (1.0 + scale_ref[...])).astype(jnp.bfloat16)

        inner = jax.nn.gelu(
            jnp.dot(norm_ref[...], up_ref[...], preferred_element_type=jnp.float32), approximate=True
        ).astype(jnp.bfloat16)
        part = jnp.dot(inner, down_ref[...], preferred_element_type=jnp.float32)

        @pl.when(j == 0)
        def _():
            acc_ref[...] = part

        @pl.when(j > 0)
        def _():
            acc_ref[...] += part

        @pl.when(j == steps - 1)
        def _():
            result = (hid_ref[...] + gate_ref[...] * acc_ref[...]).astype(jnp.bfloat16)
            out_ref[...] = result
            if with_drift:
                normed = normalize(result.astype(jnp.float32)).astype(jnp.bfloat16)
                rest[0][...] = jnp.dot(normed, fin_ref[...], preferred_element_type=jnp.float32)

    def whole(array):
        return pl.BlockSpec(array.shape, lambda j: (0,) * len(array.shape))

    out_shape = [jax.ShapeDtypeStruct((tokens, width), jnp.bfloat16)]
    if with_drift:
        out_shape.append(jax.ShapeDtypeStruct((tokens, final_weight.shape[1]), jnp.float32))
    return pl.pallas_call(
        kernel,
        grid=(steps,),
        in_specs=[
            pl.BlockSpec(memory_space=pltpu.SMEM),
            whole(patches),
            whole(received),
            whole(embed_weight),
            whole(scale),
            whole(gate),
            pl.BlockSpec((up_proj.shape[0], chunk), lambda j: (0, j)),
            pl.BlockSpec((chunk, down_proj.shape[1]), lambda j: (j, 0)),
            whole(final_weight),
        ],
        out_specs=[whole(o) for o in out_shape],
        out_shape=out_shape,
        scratch_shapes=[
            pltpu.VMEM((tokens, width), jnp.float32),
            pltpu.VMEM((tokens, width), jnp.bfloat16),
            pltpu.VMEM((tokens, width), jnp.float32),
        ],
        compiler_params=pltpu.CompilerParams(
            dimension_semantics=("arbitrary",), vmem_limit_bytes=40 * 1024 * 1024
        ),
    )(first, patches, received, embed_weight, scale, gate, up_proj, down_proj, final_weight)


def gathered_weights(weights):
    tm = lax.axis_size("tm")
    groups = lax.axis_size("groups")
    if groups != 2 or tm > 8:
        return [lax.all_gather(w, "tm", axis=0, tiled=True) for w in weights], None
    place = lax.axis_index("tm")
    mine = lax.axis_index("groups")
    halves = [w.reshape(2, w.shape[0] // 2, w.shape[1]) for w in weights]
    own = [lax.dynamic_index_in_dim(h, mine, 0, False) for h in halves]
    other = [lax.dynamic_index_in_dim(h, 1 - mine, 0, False) for h in halves]
    full = [
        lax.dynamic_update_slice(
            jnp.zeros((tm,) + h.shape, h.dtype), h[None], (place, 0, 0, 0)
        )
        for h in halves
    ]

    def put(index, piece, fallback, slot, valid, half):
        piece = jnp.where(valid, piece, fallback)
        slot = jnp.where(valid, slot, place)
        full[index] = lax.dynamic_update_slice(full[index], piece[None, None], (slot, half, 0, 0))

    ahead, behind = list(own), list(own)
    arrived = None
    for k in range(1, tm):
        right = [(i, i + 1) for i in range(k - 1, tm - 1)]
        left = [(i + 1, i) for i in range(tm - k)]
        right_ends = [j for _, j in right]
        left_ends = [j for _, j in left]
        swap_right = [(g * tm + j, (1 - g) * tm + j) for g in range(2) for j in right_ends]
        swap_left = [(g * tm + j, (1 - g) * tm + j) for g in range(2) for j in left_ends]
        for w in range(len(weights)):
            ahead[w] = lax.ppermute(ahead[w], "tm", right)
            behind[w] = lax.ppermute(behind[w], "tm", left)
            ahead_y = lax.ppermute(ahead[w], ("groups", "tm"), swap_right)
            behind_y = lax.ppermute(behind[w], ("groups", "tm"), swap_left)
            if arrived is None and w == len(weights) - 1:
                arrived = behind[w]
            has_right = place >= k
            has_left = place + k < tm
            put(w, ahead[w], own[w], place - k, has_right, mine)
            put(w, behind[w], own[w], place + k, has_left, mine)
            put(w, ahead_y, other[w], place - k, has_right, 1 - mine)
            put(w, behind_y, other[w], place + k, has_left, 1 - mine)
    return [f.reshape(-1, f.shape[-1]) for f in full], arrived


def modulation_rows(cond_rows, ada_weight):
    tm = lax.axis_size("tm")
    place = lax.axis_index("tm")
    rows = cond_rows.shape[0]
    width = ada_weight.shape[0]

    def piece(t):
        return lax.dynamic_slice(cond_rows, (0, t * width), (rows, width))

    came = [piece(place)]
    for j in range(1, tm):
        ring = [(i, (i + j) % tm) for i in range(tm)]
        came.append(lax.ppermute(piece((place + j) % tm), "tm", ring))
    partial = jnp.dot(
        jnp.concatenate(came, axis=0), ada_weight, preferred_element_type=jnp.float32
    ).reshape(tm, rows, -1)
    total = partial[0]
    for j in range(1, tm):
        total = total + lax.ppermute(partial[j], "tm", [((i + j) % tm, i) for i in range(tm)])
    return total


def shards(
    states,
    timesteps,
    step_sizes,
    labels,
    class_table,
    embed_weight,
    ada_weight,
    up_weight,
    down_weight,
    final_weight,
):
    steps_here, batch_here = states.shape[:2]
    row_total = steps_here * batch_here
    section_idx = lax.axis_index("section")
    sections = lax.axis_size("section")
    tm = lax.axis_size("tm")
    last = sections - 1
    cond_rows = condition_rows(timesteps, labels, class_table).reshape(row_total, D)
    (up_proj, down_proj), arrived = gathered_weights([up_weight[0], down_weight[0]])
    if arrived is not None:
        cond_rows, arrived = lax.optimization_barrier((cond_rows, arrived))
    modulation = modulation_rows(cond_rows, ada_weight[0])
    scale_mod = modulation[:, :D]
    gate_mod = modulation[:, D:]

    patches = states.reshape(row_total, PATCHES, PCH).astype(jnp.bfloat16)
    first = (section_idx == 0).astype(jnp.int32).reshape(1)
    received = jnp.zeros((PATCHES, D), jnp.bfloat16)
    finished = []
    for tick in range(sections + row_total - 1):
        block = jnp.clip(tick - section_idx, 0, row_total - 1)
        scale_row = lax.dynamic_slice_in_dim(scale_mod, block, 1, 0)
        gate_row = lax.dynamic_slice_in_dim(gate_mod, block, 1, 0)
        outs = layer_tick(
            first,
            patches[min(tick, row_total - 1)],
            received,
            embed_weight,
            scale_row,
            gate_row,
            up_proj,
            down_proj,
            final_weight,
            tick >= last,
        )
        leaving = outs[0]
        finished.extend(outs[1:])
        pairs = [(s, s + 1) for s in range(last) if 0 <= tick - s < row_total]
        if pairs:
            received = lax.ppermute(leaving, "section", pairs)
    drift = jnp.concatenate(finished, axis=0).reshape(steps_here, batch_here, P_SIZE)

    term_rows = step_sizes[:, None, None] * drift
    earlier = [jnp.zeros_like(term_rows[0])]
    for k in range(steps_here):
        earlier.append(earlier[-1] + term_rows[k])
    begun = jnp.where(lax.axis_index("tm") == 0, states[0], jnp.zeros_like(states[0]))
    passed = begun + earlier[-1]
    offset = begun
    for j in range(1, tm):
        pairs = [(i * sections + last, (i + j) * sections + last) for i in range(tm - j)]
        offset = offset + lax.ppermute(passed, ("tm", "section"), pairs)
    new_states = offset[None] + jnp.stack(earlier[:-1])
    step_err = jnp.max(jnp.abs(new_states - states), axis=(1, 2))

    cols = P_SIZE // sections
    err_cols = jnp.broadcast_to(step_err[:, None, None], (steps_here, batch_here, 128))

    def packed(s):
        return jnp.concatenate([new_states[:, :, s * cols : (s + 1) * cols], err_cols], axis=2)

    out = jnp.where(section_idx == last, packed(last), 0.0)
    for s in range(last):
        out = out + lax.ppermute(packed(s), "section", [(last, s)])
    return (out[:, :, :cols], out[:, 0, cols])


def solution(mesh):
    return jax.shard_map(
        shards,
        mesh=mesh,
        in_specs=(
            P(("groups", "tm"), None, None),
            P(("groups", "tm")),
            P(("groups", "tm")),
            P("groups"),
            P(),
            P(),
            P("section", "tm", None),
            P("section", "tm", None),
            P("section", "tm", None),
            P(),
        ),
        out_specs=(P(("groups", "tm"), None, "section"), P(("groups", "tm"))),
        check_vma=False,
    )
```

```python
import math

import jax
import jax.numpy as jnp
from jax import lax
from jax.experimental import pallas as pl
from jax.experimental.pallas import tpu as pltpu
from jax.sharding import PartitionSpec as P

D = 1152
PATCHES = 256
PCH = 16
P_SIZE = 4096


def condition_rows(timesteps, labels, class_table):
    half_width = D // 2
    frequency = jnp.exp(-math.log(10000.0) * jnp.arange(half_width, dtype=jnp.float32) / half_width)
    phases = timesteps.astype(jnp.float32)[:, None] * frequency[None, :]
    timing = jnp.concatenate([jnp.cos(phases), jnp.sin(phases)], axis=1)
    classes = class_table[labels].astype(jnp.float32)
    return jax.nn.silu(timing[:, None, :] + classes[None, :, :]).astype(jnp.bfloat16)


def normalize(values):
    center = values - jnp.mean(values, axis=-1, keepdims=True)
    spread = jnp.mean(center * center, axis=-1, keepdims=True)
    return center * lax.rsqrt(spread + 1e-06)


def chunk_width(total, most):
    return max(w for w in range(128, most + 1, 128) if total % w == 0)


def layer_tick(first, patches, received, embed_weight, scale, gate, up_proj, down_proj, final_weight, with_drift):
    tokens, width = received.shape
    hidden_units = up_proj.shape[1]
    chunk = chunk_width(hidden_units, 768)
    steps = hidden_units // chunk

    def kernel(first_ref, patch_ref, recv_ref, embed_ref, scale_ref, gate_ref, up_ref, down_ref, fin_ref, out_ref, *rest):
        hid_ref, norm_ref, acc_ref = rest[-3:]
        j = pl.program_id(0)

        @pl.when(j == 0)
        def _():
            embedded = jnp.dot(patch_ref[...], embed_ref[...], preferred_element_type=jnp.float32)
            hidden = jnp.where(first_ref[0] == 1, embedded, recv_ref[...].astype(jnp.float32))
            hid_ref[...] = hidden
            norm_ref[...] = (normalize(hidden) * (1.0 + scale_ref[...])).astype(jnp.bfloat16)

        inner = jax.nn.gelu(
            jnp.dot(norm_ref[...], up_ref[...], preferred_element_type=jnp.float32), approximate=True
        ).astype(jnp.bfloat16)
        part = jnp.dot(inner, down_ref[...], preferred_element_type=jnp.float32)

        @pl.when(j == 0)
        def _():
            acc_ref[...] = part

        @pl.when(j > 0)
        def _():
            acc_ref[...] += part

        @pl.when(j == steps - 1)
        def _():
            result = (hid_ref[...] + gate_ref[...] * acc_ref[...]).astype(jnp.bfloat16)
            out_ref[...] = result
            if with_drift:
                normed = normalize(result.astype(jnp.float32)).astype(jnp.bfloat16)
                rest[0][...] = jnp.dot(normed, fin_ref[...], preferred_element_type=jnp.float32)

    def whole(array):
        return pl.BlockSpec(array.shape, lambda j: (0,) * len(array.shape))

    out_shape = [jax.ShapeDtypeStruct((tokens, width), jnp.bfloat16)]
    if with_drift:
        out_shape.append(jax.ShapeDtypeStruct((tokens, final_weight.shape[1]), jnp.float32))
    return pl.pallas_call(
        kernel,
        grid=(steps,),
        in_specs=[
            pl.BlockSpec(memory_space=pltpu.SMEM),
            whole(patches),
            whole(received),
            whole(embed_weight),
            whole(scale),
            whole(gate),
            pl.BlockSpec((up_proj.shape[0], chunk), lambda j: (0, j)),
            pl.BlockSpec((chunk, down_proj.shape[1]), lambda j: (j, 0)),
            whole(final_weight),
        ],
        out_specs=[whole(o) for o in out_shape],
        out_shape=out_shape,
        scratch_shapes=[
            pltpu.VMEM((tokens, width), jnp.float32),
            pltpu.VMEM((tokens, width), jnp.bfloat16),
            pltpu.VMEM((tokens, width), jnp.float32),
        ],
        compiler_params=pltpu.CompilerParams(
            dimension_semantics=("arbitrary",), vmem_limit_bytes=40 * 1024 * 1024
        ),
    )(first, patches, received, embed_weight, scale, gate, up_proj, down_proj, final_weight)


def placed_shard(shard):
    def kernel(shard_ref, out_ref, sem):
        copy = pltpu.make_async_copy(shard_ref, out_ref.at[lax.axis_index("tm")], sem)
        copy.start()
        copy.wait()

    return pl.pallas_call(
        kernel,
        in_specs=[pl.BlockSpec(memory_space=pl.ANY)],
        out_specs=pl.BlockSpec(memory_space=pl.ANY),
        out_shape=jax.ShapeDtypeStruct((lax.axis_size("tm"),) + shard.shape, shard.dtype),
        scratch_shapes=[pltpu.SemaphoreType.DMA],
    )(shard)


def gathered_weights(weights):
    tm = lax.axis_size("tm")
    groups = lax.axis_size("groups")
    if groups != 2 or tm > 8:
        return [lax.all_gather(w, "tm", axis=0, tiled=True) for w in weights], None
    place = lax.axis_index("tm")
    mine = lax.axis_index("groups")
    halves = [w.reshape(2, w.shape[0] // 2, w.shape[1]) for w in weights]
    own = [lax.dynamic_index_in_dim(h, mine, 0, False) for h in halves]
    other = [lax.dynamic_index_in_dim(h, 1 - mine, 0, False) for h in halves]
    full = [placed_shard(h) for h in halves]

    def put(index, piece, fallback, slot, valid, half):
        piece = jnp.where(valid, piece, fallback)
        slot = jnp.where(valid, slot, place)
        full[index] = lax.dynamic_update_slice(full[index], piece[None, None], (slot, half, 0, 0))

    ahead, behind = list(own), list(own)
    arrived = None
    for k in range(1, tm):
        right = [(i, i + 1) for i in range(k - 1, tm - 1)]
        left = [(i + 1, i) for i in range(tm - k)]
        right_ends = [j for _, j in right]
        left_ends = [j for _, j in left]
        swap_right = [(g * tm + j, (1 - g) * tm + j) for g in range(2) for j in right_ends]
        swap_left = [(g * tm + j, (1 - g) * tm + j) for g in range(2) for j in left_ends]
        for w in range(len(weights)):
            ahead[w] = lax.ppermute(ahead[w], "tm", right)
            behind[w] = lax.ppermute(behind[w], "tm", left)
            ahead_y = lax.ppermute(ahead[w], ("groups", "tm"), swap_right)
            behind_y = lax.ppermute(behind[w], ("groups", "tm"), swap_left)
            if k == max(1, tm - 2):
                arrived = ahead_y
            has_right = place >= k
            has_left = place + k < tm
            put(w, ahead[w], own[w], place - k, has_right, mine)
            put(w, behind[w], own[w], place + k, has_left, mine)
            put(w, ahead_y, other[w], place - k, has_right, 1 - mine)
            put(w, behind_y, other[w], place + k, has_left, 1 - mine)
    return [f.reshape(-1, f.shape[-1]) for f in full], arrived


def modulation_rows(cond_rows, ada_weight):
    tm = lax.axis_size("tm")
    place = lax.axis_index("tm")
    rows = cond_rows.shape[0]
    width = ada_weight.shape[0]

    def piece(t):
        return lax.dynamic_slice(cond_rows, (0, t * width), (rows, width))

    came = [piece(place)]
    for j in range(1, tm):
        ring = [(i, (i + j) % tm) for i in range(tm)]
        came.append(lax.ppermute(piece((place + j) % tm), "tm", ring))
    partial = jnp.dot(
        jnp.concatenate(came, axis=0), ada_weight, preferred_element_type=jnp.float32
    ).reshape(tm, rows, -1)
    total = partial[0]
    for j in range(1, tm):
        total = total + lax.ppermute(partial[j], "tm", [((i + j) % tm, i) for i in range(tm)])
    return total


def shards(
    states,
    timesteps,
    step_sizes,
    labels,
    class_table,
    embed_weight,
    ada_weight,
    up_weight,
    down_weight,
    final_weight,
):
    steps_here, batch_here = states.shape[:2]
    row_total = steps_here * batch_here
    section_idx = lax.axis_index("section")
    sections = lax.axis_size("section")
    tm = lax.axis_size("tm")
    last = sections - 1
    cond_rows = condition_rows(timesteps, labels, class_table).reshape(row_total, D)
    (up_proj, down_proj), arrived = gathered_weights([up_weight[0], down_weight[0]])
    if arrived is not None:
        cond_rows, arrived = lax.optimization_barrier((cond_rows, arrived))
    modulation = modulation_rows(cond_rows, ada_weight[0])
    scale_mod = modulation[:, :D]
    gate_mod = modulation[:, D:]

    patches = states.reshape(row_total, PATCHES, PCH).astype(jnp.bfloat16)
    first = (section_idx == 0).astype(jnp.int32).reshape(1)
    received = jnp.zeros((PATCHES, D), jnp.bfloat16)
    finished = []
    for tick in range(sections + row_total - 1):
        block = jnp.clip(tick - section_idx, 0, row_total - 1)
        scale_row = lax.dynamic_slice_in_dim(scale_mod, block, 1, 0)
        gate_row = lax.dynamic_slice_in_dim(gate_mod, block, 1, 0)
        outs = layer_tick(
            first,
            patches[min(tick, row_total - 1)],
            received,
            embed_weight,
            scale_row,
            gate_row,
            up_proj,
            down_proj,
            final_weight,
            tick >= last,
        )
        leaving = outs[0]
        finished.extend(outs[1:])
        pairs = [(s, s + 1) for s in range(last) if 0 <= tick - s < row_total]
        if pairs:
            received = lax.ppermute(leaving, "section", pairs)
    drift = jnp.concatenate(finished, axis=0).reshape(steps_here, batch_here, P_SIZE)

    term_rows = step_sizes[:, None, None] * drift
    earlier = [jnp.zeros_like(term_rows[0])]
    for k in range(steps_here):
        earlier.append(earlier[-1] + term_rows[k])
    begun = jnp.where(lax.axis_index("tm") == 0, states[0], jnp.zeros_like(states[0]))
    passed = begun + earlier[-1]
    offset = begun
    for j in range(1, tm):
        pairs = [(i * sections + last, (i + j) * sections + last) for i in range(tm - j)]
        offset = offset + lax.ppermute(passed, ("tm", "section"), pairs)
    new_states = offset[None] + jnp.stack(earlier[:-1])
    step_err = jnp.max(jnp.abs(new_states - states), axis=(1, 2))

    cols = P_SIZE // sections
    err_cols = jnp.broadcast_to(step_err[:, None, None], (steps_here, batch_here, 128))

    def packed(s):
        return jnp.concatenate([new_states[:, :, s * cols : (s + 1) * cols], err_cols], axis=2)

    out = jnp.where(section_idx == last, packed(last), 0.0)
    for s in range(last):
        out = out + lax.ppermute(packed(s), "section", [(last, s)])
    return (out[:, :, :cols], out[:, 0, cols])


def solution(mesh):
    return jax.shard_map(
        shards,
        mesh=mesh,
        in_specs=(
            P(("groups", "tm"), None, None),
            P(("groups", "tm")),
            P(("groups", "tm")),
            P("groups"),
            P(),
            P(),
            P("section", "tm", None),
            P("section", "tm", None),
            P("section", "tm", None),
            P(),
        ),
        out_specs=(P(("groups", "tm"), None, "section"), P(("groups", "tm"))),
        check_vma=False,
    )
```
